32 devices in a mesh: slab: 2 (over x), grp: 16 (over z, y, core).
Axes of the slice: x: 2, y: 2, z: 4, core: 2. Of those that a mesh axis runs over, the one named last changes fastest.
Arguments:
- blocks: bfloat16 [128, 9, 256, 256], P(('slab', 'grp')), may hold values from -0.75 to 0.75
- diag_shift: float32 [32768], P(('slab', 'grp')), may hold values from 1 to 16
- offsets: int32 [128, 2], P(('slab', 'grp')), may hold values from 0 to 4
Outputs:
- factors: bfloat16 [128, 9, 256, 256], P(('slab', 'grp'))
The draws below stay inside these ranges and needn't reach their ends.
Inputs may be any that keep to these rules, and one draw needn't show every extreme that they name: offsets[i, 0] bounds from above the pattern's blocks left of the diagonal block of block row i and offsets[i, 1] those right of it; blocks that would lie outside the matrix are not in the pattern.
All inputs are finite; a program needn't handle non-finite values.
Results may differ from the reference program's by a relative error of at most 0.001.
Values may be sent and summed in bfloat16 or wider, within the bound.
A program may use at most 256 MiB of HBM per device.

```python
import math
import jax
import jax.numpy as jnp
from jax import lax

B = 256
BW = 4
RB = 4
ITERS = 2
NBR = 128
N_SLAB = 2
N_GRP = 16


def touch_ends(drawn, rng, least, high):
    place = [jax.random.randint(jax.random.fold_in(rng, axis), (), 0, length) for axis, length in enumerate(drawn.shape)]
    main_axis = drawn.shape.index(max(drawn.shape))
    next_to = place[:main_axis] + [(place[main_axis] + 1) % drawn.shape[main_axis]] + place[main_axis + 1:]
    return drawn.at[tuple(place)].set(least).at[tuple(next_to)].set(high)


def steps_of(stream_key, dims, split, low, largest):
    level, own = 1.0, jax.random.fold_in(stream_key, 6)
    for dim, blocks in split:
        steps = jnp.exp(jax.random.uniform(jax.random.fold_in(own, dim), (blocks,), jnp.float32, low / len(split), largest / len(split)))
        level = level * jnp.repeat(steps, dims[dim] // blocks).reshape([-1 if axis == dim else 1 for axis in range(len(dims))])
    return level


def bell_draw(rng, dims, width, reach, split=(), held_as=jnp.bfloat16):
    gain = steps_of(rng, dims, split, -0.22, 0.18) if split else 1.0
    drawn = jax.random.normal(rng, dims, jnp.float32) * width * gain
    return jnp.minimum(jnp.maximum(drawn, -reach), reach).astype(held_as)


def setup_inputs(seed: int = 0) -> dict:
    key_of = jax.random.split(jax.random.key(seed), 4)
    return {
        "blocks": bell_draw(key_of[0], (NBR, 2 * BW + 1, B, B), 0.05, 0.75, ((0, 32),)),
        "diag_shift": jnp.clip(jnp.exp(math.log(16.0) - 2.7725887 * jax.random.uniform(key_of[1], (NBR * B,), jnp.float32) ** steps_of(key_of[1], (NBR * B,), ((0, 32),), -0.2, 0.2)), 1.0, 16.0),
        "offsets": touch_ends(jax.random.randint(key_of[2], (NBR, 2), 0, BW + 1), jax.random.fold_in(key_of[2], 1), 0, BW).astype(jnp.int32),
    }


def band_pattern(global_rows, offsets, band_count, all_rows):
    band_reach = (band_count - 1) // 2
    relative = jnp.arange(band_count, dtype=jnp.int32) - band_reach
    lower_count = offsets[:, 0:1]
    upper_count = offsets[:, 1:2]
    target = global_rows[:, None] + relative[None, :]
    left_side = (relative < 0) & (-relative <= lower_count) & (target >= 0)
    right_side = (relative > 0) & (relative <= upper_count) & (target < all_rows)
    return (relative == 0) | left_side | right_side

def new_rows(factors_now, above_rows, scaled, present):
    band_count = factors_now.shape[1]
    band_reach = (band_count - 1) // 2
    row_count = factors_now.shape[0]
    block_size = factors_now.shape[2]
    partial_value = scaled.astype(jnp.float32)
    for offset_back in range(1, band_reach + 1):
        left_block = factors_now[:, band_reach - offset_back].astype(jnp.float32)
        upper_rows = above_rows[band_reach - offset_back:band_reach - offset_back + row_count, 1:].astype(jnp.float32)
        product = jnp.einsum('rab,rsbc->rsac', left_block, upper_rows)
        partial_value = partial_value.at[:, band_reach - offset_back + 1:2 * band_reach - offset_back + 1].add(-product)
    pieces = []
    for offset_back in range(band_reach, 0, -1):
        pivot_block = above_rows[band_reach - offset_back:band_reach - offset_back + row_count, 0].astype(jnp.float32)
        strict = jnp.triu(pivot_block, 1)
        inner_term = jnp.einsum('rab,rbc->rac', factors_now[:, band_reach - offset_back].astype(jnp.float32), strict)
        diag_values = jnp.diagonal(pivot_block, axis1=1, axis2=2)
        divisor = jnp.where(present[:, band_reach - offset_back][:, None], diag_values, 1.0)
        pieces.append((partial_value[:, band_reach - offset_back] - inner_term) / divisor[:, None, :])
    own_block = factors_now[:, band_reach].astype(jnp.float32)
    strict_lower = jnp.tril(own_block, -1)
    diag_rest = partial_value[:, band_reach] - jnp.einsum('rab,rbc->rac', strict_lower, jnp.triu(own_block, 1))
    own_diag = jnp.diagonal(own_block, axis1=1, axis2=2)
    below_mask = jnp.tril(jnp.ones((block_size, block_size), jnp.int32), -1) > 0
    pieces.append(jnp.where(below_mask[None], diag_rest / own_diag[:, None, :], diag_rest))
    upper_terms = partial_value[:, band_reach + 1:] - jnp.einsum('rab,rsbc->rsac', strict_lower, factors_now[:, band_reach + 1:].astype(jnp.float32))
    stacked = jnp.concatenate([jnp.stack(pieces, 1), upper_terms], 1)
    return jnp.where(present[:, :, None, None], stacked, 0.0).astype(jnp.bfloat16)

def reference(blocks, diag_shift, offsets):
    row_total, band_count, block_size, _ = blocks.shape
    band_reach = (band_count - 1) // 2
    shift_rows = diag_shift.reshape(row_total, block_size)
    diag_values = shift_rows + jnp.diagonal(blocks[:, band_reach].astype(jnp.float32), axis1=1, axis2=2)
    padded = jnp.pad(diag_values, ((band_reach, band_reach), (0, 0)))
    positive = padded > 0
    scales = jnp.where(positive, 1.0 / jnp.sqrt(jnp.where(positive, padded, 1.0)), 0.0)
    row_scale = scales[band_reach:band_reach + row_total]
    col_scale = jnp.stack([scales[column:column + row_total] for column in range(band_count)], 1)
    present = band_pattern(jnp.arange(row_total, dtype=jnp.int32), offsets, band_count, row_total)
    group_count = row_total // RB
    identity = jnp.eye(block_size, dtype=jnp.float32)

    def scale_group(index):
        start = (index * RB).astype(jnp.int32)
        piece = lax.dynamic_slice_in_dim(blocks, start, RB, 0).astype(jnp.float32)
        added = lax.dynamic_slice_in_dim(shift_rows, start, RB, 0)
        piece = piece.at[:, band_reach].add(identity[None] * added[:, None, :])
        rscale = lax.dynamic_slice_in_dim(row_scale, start, RB, 0)
        cscale = lax.dynamic_slice_in_dim(col_scale, start, RB, 0)
        marks = lax.dynamic_slice_in_dim(present, start, RB, 0)
        value = piece * rscale[:, None, :, None] * cscale[:, :, None, :]
        return jnp.where(marks[:, :, None, None], value, 0.0).astype(jnp.bfloat16)
    scaled = lax.map(scale_group, jnp.arange(group_count, dtype=jnp.int32)).reshape(blocks.shape)
    padded_state = jnp.concatenate([jnp.zeros((band_reach,) + blocks.shape[1:], jnp.bfloat16), scaled], 0)
    slab_rows = N_GRP * RB

    def slab_update(slab_index, padded_state):
        slab_start = (slab_index * slab_rows).astype(jnp.int32)

        def group_update(group_index):
            start = (slab_start + group_index * RB).astype(jnp.int32)
            current = lax.dynamic_slice_in_dim(padded_state, start + band_reach, RB, 0)
            above_rows = lax.dynamic_slice_in_dim(padded_state, start, RB + band_reach, 0)[:, band_reach:]
            return new_rows(current, above_rows, lax.dynamic_slice_in_dim(scaled, start, RB, 0), lax.dynamic_slice_in_dim(present, start, RB, 0))
        fresh = lax.map(group_update, jnp.arange(N_GRP, dtype=jnp.int32)).reshape((slab_rows,) + blocks.shape[1:])
        return lax.dynamic_update_slice_in_dim(padded_state, fresh, (slab_start + band_reach).astype(jnp.int32), 0)
    for sweep_index in range(ITERS):
        padded_state = lax.fori_loop(0, N_SLAB, slab_update, padded_state)
    return padded_state[band_reach:]
```

```python
import functools

import jax
import jax.numpy as jnp
from jax import lax
from jax.experimental import pallas as pl
from jax.experimental.pallas import tpu as pltpu
from jax.sharding import PartitionSpec as P

MESH = pl.DeviceIdType.MESH
F32 = jnp.float32
BF16 = jnp.bfloat16

DIAG, SHIFT, UPPER, LOWER, SENT = 0, 1, 2, 8, 8


def band_pattern(global_rows, offsets, band_count, all_rows):
    band_reach = (band_count - 1) // 2
    relative = jnp.arange(band_count, dtype=jnp.int32) - band_reach
    lower_count = offsets[:, 0:1]
    upper_count = offsets[:, 1:2]
    target = global_rows[:, None] + relative[None, :]
    left_side = (relative < 0) & (-relative <= lower_count) & (target >= 0)
    right_side = (relative > 0) & (relative <= upper_count) & (target < all_rows)
    return (relative == 0) | left_side | right_side


def kernel(
    slabs, groups, reach,
    blocks, aux, out,
    blk, aux_own, aux_prev, aux_next, scale, a, w1, w2, low2, h1, f2,
    load_sem, aux_load_sem, out_sem, aux_send, aux_recv, send1, recv1, send2, recv2,
):
    rows, band, size, _ = blk.shape
    slab, grp = lax.axis_index("slab"), lax.axis_index("grp")
    here = slab * groups + grp
    has_prev = here > 0
    has_next = here < slabs * groups - 1
    after = lax.rem(here + 1, slabs * groups)
    before = lax.rem(here + slabs * groups - 1, slabs * groups)
    nxt = (lax.div(after, groups), lax.rem(after, groups))
    prv = (lax.div(before, groups), lax.rem(before, groups))
    inner = grp < groups - 1
    edge = jnp.logical_and(grp == groups - 1, has_next)

    def copy1(j, src):
        return pltpu.make_async_remote_copy(
            src_ref=src, dst_ref=h1.at[j], send_sem=send1.at[j], recv_sem=recv1.at[j],
            device_id=nxt, device_id_type=MESH,
        )

    def copy2(j, src):
        return pltpu.make_async_remote_copy(
            src_ref=src, dst_ref=w2.at[j], send_sem=send2.at[j], recv_sem=recv2.at[j],
            device_id=nxt, device_id_type=MESH,
        )

    def load(j):
        return pltpu.make_async_copy(blocks.at[j], blk.at[j], load_sem.at[j])

    def raw_upper(j):
        return blocks.at[j, pl.ds(reach, reach + 1)]

    aux_head = aux.at[:, pl.ds(0, SENT)]
    to_next = pltpu.make_async_remote_copy(
        src_ref=aux_head, dst_ref=aux_prev, send_sem=aux_send.at[0], recv_sem=aux_recv.at[0],
        device_id=nxt, device_id_type=MESH,
    )
    to_prev = pltpu.make_async_remote_copy(
        src_ref=aux_head, dst_ref=aux_next, send_sem=aux_send.at[1], recv_sem=aux_recv.at[1],
        device_id=prv, device_id_type=MESH,
    )
    aux_load = pltpu.make_async_copy(aux, aux_own, aux_load_sem.at[0])

    aux_load.start()
    for j in range(rows):
        load(j).start()

    barrier = pltpu.get_barrier_semaphore()

    @pl.when(has_prev)
    def _():
        pl.semaphore_signal(barrier, inc=1, device_id=prv, device_id_type=MESH)

    @pl.when(has_next)
    def _():
        pl.semaphore_signal(barrier, inc=1, device_id=nxt, device_id_type=MESH)

    pl.semaphore_wait(barrier, has_prev.astype(jnp.int32) + has_next.astype(jnp.int32))

    @pl.when(has_prev)
    def _():
        to_prev.start()

    @pl.when(has_next)
    def _():
        to_next.start()

    @pl.when(inner)
    def _():
        for j in reversed(range(rows)):
            copy1(j, raw_upper(j)).start()

    row_id = lax.broadcasted_iota(jnp.int32, (size, size), 0)
    col_id = lax.broadcasted_iota(jnp.int32, (size, size), 1)
    eye = row_id == col_id

    def scale_of(values):
        positive = values > 0
        return jnp.where(positive, 1.0 / jnp.sqrt(jnp.where(positive, values, 1.0)), 0.0)

    def as_column(row):
        return jnp.sum(jnp.where(eye, row, 0.0), axis=1, keepdims=True)

    @pl.when(jnp.logical_not(has_prev))
    def _():
        aux_prev[...] = jnp.zeros_like(aux_prev)
        for j in range(reach):
            for k in range(reach + 1):
                w1[j, k] = jnp.zeros((size, size), BF16)
                w2[j, k] = jnp.zeros((size, size), BF16)

    @pl.when(jnp.logical_not(has_next))
    def _():
        aux_next[...] = jnp.zeros_like(aux_next)

    aux_load.wait()

    @pl.when(has_prev)
    def _():
        to_next.wait_recv()

    @pl.when(has_next)
    def _():
        to_prev.wait_recv()

    for j in range(rows):
        scale[j] = scale_of(aux_prev[j, DIAG : DIAG + 1, :])
        scale[rows + j] = scale_of(aux_own[j, DIAG : DIAG + 1, :])
        scale[2 * rows + j] = scale_of(aux_next[j, DIAG : DIAG + 1, :])

    def mask_of(table, j, k):
        place = UPPER + k - reach if k >= reach else LOWER + k
        return table[j, place : place + 1, :] > 0.5

    def scaled_block(block, table, j, k, shift, left, right):
        value = block.astype(F32)
        if k == reach:
            value = value + jnp.where(eye, shift, 0.0)
        value = value * left * right
        return jnp.where(mask_of(table, j, k), value, 0.0).astype(BF16)

    def scale_own(j, carry):
        load(j).wait()
        left = as_column(scale[rows + j])
        shift = aux_own[j, SHIFT : SHIFT + 1, :]
        for k in range(band):
            value = scaled_block(blk[j, k], aux_own, j, k, shift, left, scale[j + k])
            a[j, k] = value
            if k >= reach:
                w1[reach + j, k - reach] = value
        return carry

    lax.fori_loop(0, rows, scale_own, 0)

    def update(j, low, w, put):
        def dot(x, y):
            return jnp.dot(x, y, preferred_element_type=F32)

        def partial(k):
            total = a[j, k].astype(F32)
            for m in range(1, reach + 1):
                s = k - reach + m
                if 1 <= s <= reach:
                    total = total - dot(low[j, reach - m], w[reach + j - m, s])
            return total

        def finish(k, value):
            put(k, jnp.where(mask_of(aux_own, j, k), value, 0.0).astype(BF16))

        own = w[reach + j, 0].astype(F32)
        below = row_id > col_id
        strict_low = jnp.where(below, own, 0.0).astype(BF16)
        for k in range(reach + 1, band):
            finish(k, partial(k) - dot(strict_low, w[reach + j, k - reach]))
        strict_up = jnp.where(row_id < col_id, own, 0.0).astype(BF16)
        rest = partial(reach) - dot(strict_low, strict_up)
        pivots = jnp.sum(jnp.where(eye, own, 0.0), axis=0, keepdims=True)
        finish(reach, jnp.where(below, rest / pivots, rest))
        for k in range(reach):
            m = reach - k
            pivot = w[reach + j - m, 0].astype(F32)
            strict = jnp.where(row_id < col_id, pivot, 0.0).astype(BF16)
            rest = partial(k) - dot(low[j, k], strict)
            pivots = jnp.sum(jnp.where(eye, pivot, 0.0), axis=0, keepdims=True)
            divisor = jnp.where(mask_of(aux_own, j, k), pivots, 1.0)
            finish(k, rest / divisor)

    def first_sweep(i, carry):
        j = rows - 1 - i

        @pl.when(has_prev)
        def _():
            copy1(j, w2.at[reach + j]).wait_recv()

        @pl.when(grp > 0)
        def _():
            left = as_column(scale[j])
            shift = aux_prev[j, SHIFT : SHIFT + 1, :]
            for k in range(reach + 1):
                w1[j, k] = scaled_block(
                    h1[j, k], aux_prev, j, reach + k, shift, left, scale[j + k]
                )

        @pl.when(jnp.logical_and(grp == 0, has_prev))
        def _():
            for k in range(reach + 1):
                w1[j, k] = h1[j, k]

        def put(k, value):
            if k >= reach:
                w2[reach + j, k - reach] = value
            else:
                low2[j, k] = value

        update(j, a, w1, put)

        @pl.when(inner)
        def _():
            copy2(j, w2.at[reach + j]).start()

        @pl.when(edge)
        def _():
            copy1(j, w2.at[reach + j]).start()

        return carry

    lax.fori_loop(0, rows, first_sweep, 0)

    def second_sweep(i, carry):
        j = rows - 1 - i

        @pl.when(has_prev)
        def _():
            copy2(j, w2.at[reach + j]).wait_recv()

        def put(k, value):
            f2[j, k] = value

        update(j, low2, w2, put)

        @pl.when(edge)
        def _():
            copy2(j, f2.at[j, pl.ds(reach, reach + 1)]).start()

        pltpu.make_async_copy(f2.at[j], out.at[j], out_sem.at[j]).start()
        return carry

    lax.fori_loop(0, rows, second_sweep, 0)

    for j in range(rows):
        pltpu.make_async_copy(f2.at[j], out.at[j], out_sem.at[j]).wait()

    @pl.when(has_next)
    def _():
        to_next.wait_send()
        for j in range(rows):
            copy1(j, w2.at[reach + j]).wait_send()
            copy2(j, w2.at[reach + j]).wait_send()

    @pl.when(has_prev)
    def _():
        to_prev.wait_send()


def per_device(blocks, diag_shift, offsets):
    rows, band, size, _ = blocks.shape
    reach = (band - 1) // 2
    assert rows == reach and reach <= 4
    slabs, groups = lax.axis_size("slab"), lax.axis_size("grp")
    first_row = (lax.axis_index("slab") * groups + lax.axis_index("grp")) * rows
    shift = diag_shift.reshape(rows, size)
    eye = jnp.eye(size, dtype=bool)
    diagonal = jnp.sum(jnp.where(eye[None], blocks[:, reach].astype(F32), 0.0), axis=1)
    present = band_pattern(
        first_row + jnp.arange(rows, dtype=jnp.int32), offsets, band, rows * slabs * groups
    ).astype(F32)
    marks = jnp.broadcast_to(present[:, :, None], (rows, band, size))
    pieces = [(shift + diagonal)[:, None], shift[:, None], marks[:, reach:]]
    pieces.append(jnp.zeros((rows, LOWER - UPPER - reach - 1, size), F32))
    pieces.append(marks[:, :reach])
    pieces.append(jnp.zeros((rows, 16 - LOWER - reach, size), F32))
    aux = jnp.concatenate(pieces, axis=1)

    block = (size, size)
    upper = (reach + 1,) + block
    dma = pltpu.SemaphoreType.DMA
    return pl.pallas_call(
        functools.partial(kernel, slabs, groups, reach),
        out_shape=jax.ShapeDtypeStruct(blocks.shape, BF16),
        in_specs=[pl.BlockSpec(memory_space=pl.ANY)] * 2,
        out_specs=pl.BlockSpec(memory_space=pl.ANY),
        scratch_shapes=[
            pltpu.VMEM(blocks.shape, BF16),
            pltpu.VMEM(aux.shape, F32),
            pltpu.VMEM((rows, SENT, size), F32),
            pltpu.VMEM((rows, SENT, size), F32),
            pltpu.VMEM((3 * rows, 1, size), F32),
            pltpu.VMEM(blocks.shape, BF16),
            pltpu.VMEM((reach + rows,) + upper, BF16),
            pltpu.VMEM((reach + rows,) + upper, BF16),
            pltpu.VMEM((rows, reach) + block, BF16),
            pltpu.VMEM((rows,) + upper, BF16),
            pltpu.VMEM(blocks.shape, BF16),
            dma((rows,)), dma((1,)), dma((rows,)), dma((2,)), dma((2,)),
            dma((rows,)), dma((rows,)), dma((rows,)), dma((rows,)),
        ],
        compiler_params=pltpu.CompilerParams(collective_id=0, has_side_effects=True),
    )(blocks, aux)


def solution(mesh):
    return jax.shard_map(
        per_device,
        mesh=mesh,
        in_specs=(
            P(("slab", "grp"), None, None, None),
            P(("slab", "grp")),
            P(("slab", "grp"), None),
        ),
        out_specs=P(("slab", "grp"), None, None, None),
        check_vma=False,
    )
```

```python
import functools

import jax
import jax.numpy as jnp
from jax import lax
from jax.experimental import pallas as pl
from jax.experimental.pallas import tpu as pltpu
from jax.sharding import PartitionSpec as P

MESH = pl.DeviceIdType.MESH
F32 = jnp.float32
BF16 = jnp.bfloat16

DIAG, SHIFT, UPPER, LOWER, SENT = 0, 1, 2, 8, 8


def kernel(
    slabs, groups, reach,
    blocks, shifts, offsets, f2,
    blk, shift_own, aux_own, aux_prev, aux_next, scale, a, w1, w2, low2, h1,
    load_sem, aux_load_sem, aux_send, aux_recv, send1, recv1, send2, recv2,
):
    rows, band, size, _ = blk.shape
    slab, grp = lax.axis_index("slab"), lax.axis_index("grp")
    here = slab * groups + grp
    has_prev = here > 0
    has_next = here < slabs * groups - 1
    after = lax.rem(here + 1, slabs * groups)
    before = lax.rem(here + slabs * groups - 1, slabs * groups)
    nxt = (lax.div(after, groups), lax.rem(after, groups))
    prv = (lax.div(before, groups), lax.rem(before, groups))
    inner = grp < groups - 1
    edge = jnp.logical_and(grp == groups - 1, has_next)

    half = size // 2

    def pieces(src, dst, send, recv):
        top, low = pl.ds(0, half), pl.ds(half, half)
        cuts = ((0, top), (0, low, low), (pl.ds(1, reach),))
        return [
            pltpu.make_async_remote_copy(
                src_ref=src.at[cut], dst_ref=dst.at[cut],
                send_sem=send.at[n], recv_sem=recv.at[n],
                device_id=nxt, device_id_type=MESH,
            )
            for n, cut in enumerate(cuts)
        ]

    def copy1(j, src):
        return pieces(src, h1.at[j], send1.at[j], recv1.at[j])

    def copy2(j, src):
        return pieces(src, w2.at[j], send2.at[j], recv2.at[j])

    def start(copies):
        for copy in copies:
            copy.start()

    def wait_send(copies):
        for copy in copies:
            copy.wait_send()

    def wait_recv(copies):
        for copy in copies:
            copy.wait_recv()

    def load(j):
        others = (pl.ds(0, reach), pl.ds(reach + 1, reach))
        return [
            pltpu.make_async_copy(blocks.at[j, cut], blk.at[j, cut], load_sem.at[j, n])
            for n, cut in enumerate(others)
        ]

    def load_diagonal(j):
        return pltpu.make_async_copy(
            blocks.at[j, reach], blk.at[j, reach], load_sem.at[j, 2]
        )

    def raw_upper(j):
        return blocks.at[j, pl.ds(reach, reach + 1)]

    aux_head = aux_own.at[:, pl.ds(0, SENT)]
    to_next = pltpu.make_async_remote_copy(
        src_ref=aux_head, dst_ref=aux_prev, send_sem=aux_send.at[0], recv_sem=aux_recv.at[0],
        device_id=nxt, device_id_type=MESH,
    )
    to_prev = pltpu.make_async_remote_copy(
        src_ref=aux_head, dst_ref=aux_next, send_sem=aux_send.at[1], recv_sem=aux_recv.at[1],
        device_id=prv, device_id_type=MESH,
    )
    shift_load = pltpu.make_async_copy(shifts, shift_own, aux_load_sem.at[0])

    shift_load.start()
    for j in range(rows):
        load_diagonal(j).start()
    for j in range(rows):
        start(load(j))

    barrier = pltpu.get_barrier_semaphore()

    @pl.when(has_prev)
    def _():
        pl.semaphore_signal(barrier, inc=1, device_id=prv, device_id_type=MESH)

    @pl.when(has_next)
    def _():
        pl.semaphore_signal(barrier, inc=1, device_id=nxt, device_id_type=MESH)

    pl.semaphore_wait(barrier, has_prev.astype(jnp.int32) + has_next.astype(jnp.int32))

    @pl.when(inner)
    def _():
        for j in reversed(range(rows)):
            start(copy1(j, raw_upper(j)))

    row_id = lax.broadcasted_iota(jnp.int32, (size, size), 0)
    col_id = lax.broadcasted_iota(jnp.int32, (size, size), 1)
    eye = row_id == col_id

    def scale_of(values):
        positive = values > 0
        return jnp.where(positive, 1.0 / jnp.sqrt(jnp.where(positive, values, 1.0)), 0.0)

    def as_column(row):
        return jnp.sum(jnp.where(eye, row, 0.0), axis=1, keepdims=True)

    @pl.when(jnp.logical_not(has_prev))
    def _():
        aux_prev[...] = jnp.zeros_like(aux_prev)
        for j in range(reach):
            for k in range(reach + 1):
                w1[j, k] = jnp.zeros((size, size), BF16)
                w2[j, k] = jnp.zeros((size, size), BF16)

    @pl.when(jnp.logical_not(has_next))
    def _():
        aux_next[...] = jnp.zeros_like(aux_next)

    shift_load.wait()
    for j in range(rows):
        load_diagonal(j).wait()
        diagonal = jnp.sum(
            jnp.where(eye, blk[j, reach].astype(F32), 0.0), axis=0, keepdims=True
        )
        aux_own[j, DIAG : DIAG + 1, :] = shift_own[j] + diagonal
        aux_own[j, SHIFT : SHIFT + 1, :] = shift_own[j]
        row = here * rows + j
        for k in range(band):
            away = abs(k - reach)
            if k < reach:
                count = jnp.where(row - away >= 0, offsets[j, 0], 0)
            else:
                count = jnp.where(row + away < slabs * groups * rows, offsets[j, 1], 0)
            marks = jnp.where(jnp.full((1, size), count, jnp.int32) >= away, 1.0, 0.0)
            place = UPPER + k - reach if k >= reach else LOWER + k
            aux_own[j, place : place + 1, :] = marks
        if UPPER + reach + 1 < LOWER:
            spare = LOWER - UPPER - reach - 1
            aux_own[j, UPPER + reach + 1 : LOWER, :] = jnp.zeros((spare, size), F32)

    @pl.when(has_next)
    def _():
        to_next.start()

    @pl.when(has_prev)
    def _():
        to_prev.start()

    @pl.when(has_prev)
    def _():
        to_next.wait_recv()

    @pl.when(has_next)
    def _():
        to_prev.wait_recv()

    for j in range(rows):
        scale[j] = scale_of(aux_prev[j, DIAG : DIAG + 1, :])
        scale[rows + j] = scale_of(aux_own[j, DIAG : DIAG + 1, :])
        scale[2 * rows + j] = scale_of(aux_next[j, DIAG : DIAG + 1, :])

    def mask_of(table, j, k):
        place = UPPER + k - reach if k >= reach else LOWER + k
        return table[j, place : place + 1, :] > 0.5

    def scaled_block(block, table, j, k, shift, left, right):
        value = block.astype(F32)
        if k == reach:
            value = value + jnp.where(eye, shift, 0.0)
        value = value * left * right
        return jnp.where(mask_of(table, j, k), value, 0.0).astype(BF16)

    def scale_own(j, carry):
        for copy in load(j):
            copy.wait()
        left = as_column(scale[rows + j])
        shift = aux_own[j, SHIFT : SHIFT + 1, :]
        for k in range(band):
            value = scaled_block(blk[j, k], aux_own, j, k, shift, left, scale[j + k])
            a[j, k] = value
            if k >= reach:
                w1[reach + j, k - reach] = value
        return carry

    lax.fori_loop(0, rows, scale_own, 0)

    def update(j, low, w, put):
        def dot(x, y):
            return jnp.dot(x, y, preferred_element_type=F32)

        def partial(k):
            total = a[j, k].astype(F32)
            for m in range(1, reach + 1):
                s = k - reach + m
                if 1 <= s <= reach:
                    total = total - dot(low[j, reach - m], w[reach + j - m, s])
            return total

        def finish(k, value):
            put(k, jnp.where(mask_of(aux_own, j, k), value, 0.0).astype(BF16))

        own = w[reach + j, 0].astype(F32)
        below = row_id > col_id
        strict_low = jnp.where(below, own, 0.0).astype(BF16)
        for k in range(reach + 1, band):
            finish(k, partial(k) - dot(strict_low, w[reach + j, k - reach]))
        strict_up = jnp.where(row_id < col_id, own, 0.0).astype(BF16)
        rest = partial(reach) - dot(strict_low, strict_up)
        pivots = jnp.sum(jnp.where(eye, own, 0.0), axis=0, keepdims=True)
        finish(reach, jnp.where(below, rest / pivots, rest))
        for k in range(reach):
            m = reach - k
            pivot = w[reach + j - m, 0].astype(F32)
            strict = jnp.where(row_id < col_id, pivot, 0.0).astype(BF16)
            rest = partial(k) - dot(low[j, k], strict)
            pivots = jnp.sum(jnp.where(eye, pivot, 0.0), axis=0, keepdims=True)
            divisor = jnp.where(mask_of(aux_own, j, k), pivots, 1.0)
            finish(k, rest / divisor)

    def first_sweep(i, carry):
        j = rows - 1 - i

        @pl.when(has_prev)
        def _():
            wait_recv(copy1(j, w2.at[reach + j]))

        @pl.when(grp > 0)
        def _():
            left = as_column(scale[j])
            shift = aux_prev[j, SHIFT : SHIFT + 1, :]
            for k in range(reach + 1):
                w1[j, k] = scaled_block(
                    h1[j, k], aux_prev, j, reach + k, shift, left, scale[j + k]
                )

        @pl.when(jnp.logical_and(grp == 0, has_prev))
        def _():
            for k in range(reach + 1):
                w1[j, k] = h1[j, k]

        def put(k, value):
            if k >= reach:
                w2[reach + j, k - reach] = value
            else:
                low2[j, k] = value

        update(j, a, w1, put)

        @pl.when(inner)
        def _():
            start(copy2(j, w2.at[reach + j]))

        @pl.when(edge)
        def _():
            start(copy1(j, w2.at[reach + j]))

        return carry

    lax.fori_loop(0, rows, first_sweep, 0)

    def second_sweep(i, carry):
        j = rows - 1 - i

        @pl.when(has_prev)
        def _():
            wait_recv(copy2(j, w2.at[reach + j]))

        def put(k, value):
            f2[j, k] = value

        update(j, low2, w2, put)

        @pl.when(edge)
        def _():
            start(copy2(j, f2.at[j, pl.ds(reach, reach + 1)]))

        return carry

    lax.fori_loop(0, rows, second_sweep, 0)

    @pl.when(has_next)
    def _():
        to_next.wait_send()
        for j in range(rows):
            wait_send(copy1(j, w2.at[reach + j]))
            wait_send(copy2(j, w2.at[reach + j]))

    @pl.when(has_prev)
    def _():
        to_prev.wait_send()


def per_device(blocks, diag_shift, offsets):
    rows, band, size, _ = blocks.shape
    reach = (band - 1) // 2
    assert rows == reach and reach <= 4
    slabs, groups = lax.axis_size("slab"), lax.axis_size("grp")
    shift = diag_shift.reshape(rows, 1, size)
    block = (size, size)
    upper = (reach + 1,) + block
    dma = pltpu.SemaphoreType.DMA
    return pl.pallas_call(
        functools.partial(kernel, slabs, groups, reach),
        out_shape=pltpu.VMEM(blocks.shape, BF16),
        in_specs=[
            pl.BlockSpec(memory_space=pltpu.HBM),
            pl.BlockSpec(memory_space=pltpu.HBM),
            pl.BlockSpec(memory_space=pltpu.SMEM),
        ],
        out_specs=pl.BlockSpec(memory_space=pltpu.VMEM),
        scratch_shapes=[
            pltpu.VMEM(blocks.shape, BF16),
            pltpu.VMEM((rows, 1, size), F32),
            pltpu.VMEM((rows, 2 * SENT, size), F32),
            pltpu.VMEM((rows, SENT, size), F32),
            pltpu.VMEM((rows, SENT, size), F32),
            pltpu.VMEM((3 * rows, 1, size), F32),
            pltpu.VMEM(blocks.shape, BF16),
            pltpu.VMEM((reach + rows,) + upper, BF16),
            pltpu.VMEM((reach + rows,) + upper, BF16),
            pltpu.VMEM((rows, reach) + block, BF16),
            pltpu.VMEM((rows,) + upper, BF16),
            dma((rows, 3)), dma((1,)), dma((2,)), dma((2,)),
            dma((rows, 3)), dma((rows, 3)), dma((rows, 3)), dma((rows, 3)),
        ],
        compiler_params=pltpu.CompilerParams(collective_id=0, has_side_effects=True, vmem_limit_bytes=57 << 20),
    )(blocks, shift, offsets)


def solution(mesh):
    return jax.shard_map(
        per_device,
        mesh=mesh,
        in_specs=(
            P(("slab", "grp"), None, None, None),
            P(("slab", "grp")),
            P(("slab", "grp"), None),
        ),
        out_specs=P(("slab", "grp"), None, None, None),
        check_vma=False,
    )
```
